128 devices in a mesh: dp: 1, sp: 64 (over z, y, x), cp: 2 (over core).
Axes of the slice: x: 4, y: 4, z: 4, core: 2. Of those that a mesh axis runs over, the one named last changes fastest.
Arguments:
- x_act: bfloat16 [16, 128, 7, 2048], P('dp', 'sp', None, 'cp')
- w_one: bfloat16 [3, 3, 2048, 8192], P(None, None, 'cp')
- w_two: bfloat16 [3, 3, 8192, 2048], P(None, None, 'cp')
- bias_one: float32 [8192], replicated
Outputs:
- output: bfloat16 [16, 128, 7, 2048], P('dp', 'sp', None, 'cp')
All inputs are finite; a program needn't handle non-finite values.
Results may differ from the reference program's by a relative error of at most 0.001.
Values are sent between devices in bfloat16 or wider.
A program may use at most 1.25 GiB of HBM per device.

```python
import jax
import jax.numpy as jnp
from jax import lax

BATCH_SIZE = 16
GRID_ROWS = 128
GRID_COLS = 7
CHANNELS = 2048
HIDDEN_CHANNELS = 4 * CHANNELS
CONV_DIMS = ("NHWC", "HWIO", "NHWC")


def setup_inputs(seed: int = 0, part: int = 0) -> dict:
    base_key = jax.random.key(seed)
    key_x, key_one, key_two, key_bias = jax.random.split(base_key, 4)
    x_act = jax.random.normal(jax.random.fold_in(key_x, part), (BATCH_SIZE, GRID_ROWS, GRID_COLS, CHANNELS), jnp.float32)
    w_one = jax.random.normal(key_one, (3, 3, CHANNELS, HIDDEN_CHANNELS), jnp.float32) * (9 * CHANNELS) ** -0.5
    w_two = jax.random.normal(key_two, (3, 3, HIDDEN_CHANNELS, CHANNELS), jnp.float32) * (9 * HIDDEN_CHANNELS) ** -0.5
    bias_one = 0.7 * jax.random.normal(key_bias, (HIDDEN_CHANNELS,), jnp.float32)
    return {"x_act": x_act.astype(jnp.bfloat16), "w_one": w_one.astype(jnp.bfloat16), "w_two": w_two.astype(jnp.bfloat16), "bias_one": bias_one}


def reference(x_act, w_one, w_two, bias_one):
    w_first = w_one.astype(jnp.float32)
    w_second = w_two.astype(jnp.float32)

    def one_picture(picture):
        pic_f32 = picture.astype(jnp.float32)[None]
        pre_act = lax.conv_general_dilated(pic_f32, w_first, (1, 1), "SAME", dimension_numbers=CONV_DIMS)
        hidden = jax.nn.relu(pre_act + bias_one).astype(jnp.bfloat16)
        post_act = lax.conv_general_dilated(hidden.astype(jnp.float32), w_second, (1, 1), "SAME", dimension_numbers=CONV_DIMS)
        return (pic_f32 + post_act)[0].astype(jnp.bfloat16)

    return lax.map(one_picture, x_act)
```

```python
import functools

import jax
import jax.numpy as jnp
from jax import lax
from jax.experimental import pallas as pl
from jax.experimental.pallas import tpu as pltpu
from jax.sharding import PartitionSpec as P

IMAGES = 16
COLS = 7
ROW = COLS * IMAGES
OWN = 2 * ROW
CHUNK = 512
KBLOCK = 1024
KY_ORDER = (1, 0, 2)
MESH = pl.DeviceIdType.MESH


def resblock_kernel(sp_size, chan, hidden, x_ref, w1_ref, w2_ref, bias_ref, out_ref,
                    xbuf, abuf, wbuf, acc, send, recv1, recv2, bias_v,
                    wsem, xsem, bsem, xs_sem, xr_sem, ps_sem, pr1_sem, pr2_sem, hs_sem, hr_sem):
    c = lax.axis_index("cp")
    s = lax.axis_index("sp")
    other = 1 - c
    up = lax.rem(s + sp_size - 1, sp_size)
    down = lax.rem(s + 1, sp_size)
    has_up = s > 0
    has_down = s < sp_size - 1
    half_h = hidden // 2
    half_o = chan // 2
    n1 = half_h // CHUNK
    n2 = half_o // CHUNK
    kb2 = half_h // KBLOCK
    groups1 = 2 * n1
    groups = groups1 + 2 * n2 * kb2
    slots = wbuf.shape[0]

    def w_copy(ref, rows, cols, slot, i):
        ky = KY_ORDER[i]
        return pltpu.make_async_copy(
            ref.at[pl.ds(3 * ky, 3), pl.ds(rows, KBLOCK), pl.ds(cols, CHUNK)],
            wbuf.at[slot, i], wsem.at[slot, i])

    def fetch(g):
        slot = lax.rem(g, slots)

        @pl.when(g < groups1)
        def _():
            side = lax.rem(g, 2)
            cols = (side * c + (1 - side) * other) * half_h + (g // 2) * CHUNK
            for i in range(3):
                w_copy(w1_ref, 0, pl.multiple_of(cols, CHUNK), slot, i).start()

        @pl.when((g >= groups1) & (g < groups))
        def _():
            t = g - groups1
            m = t // kb2
            kb = lax.rem(t, kb2)
            side = m // n2
            cols = (side * c + (1 - side) * other) * half_o + lax.rem(m, n2) * CHUNK
            rows = pl.multiple_of(kb * KBLOCK, KBLOCK)
            for i in range(3):
                w_copy(w2_ref, rows, pl.multiple_of(cols, CHUNK), slot, i).start()

    def x_send(i):
        src = x_ref.at[pl.ds(i * ROW, ROW)]
        dst = xbuf.at[3 if i == 0 else 0, pl.ds(IMAGES, ROW)]
        return pltpu.make_async_remote_copy(
            src, dst, xs_sem.at[i], xr_sem.at[i],
            device_id={"sp": up if i == 0 else down}, device_id_type=MESH)

    def halo_send(i, j):
        src = abuf.at[j, 1 + i, pl.ds(IMAGES, ROW)]
        dst = abuf.at[j, 3 if i == 0 else 0, pl.ds(IMAGES, ROW)]
        return pltpu.make_async_remote_copy(
            src, dst, hs_sem.at[i, j], hr_sem.at[i, j],
            device_id={"sp": up if i == 0 else down}, device_id_type=MESH)

    def part_send(slot, dst, rsem):
        return pltpu.make_async_remote_copy(
            send.at[slot], dst, ps_sem.at[slot], rsem,
            device_id={"cp": other}, device_id_type=MESH)

    for g in range(slots):
        fetch(jnp.int32(g))
    x_copies = [pltpu.make_async_copy(x_ref.at[pl.ds(h * ROW, ROW)], xbuf.at[1 + h, pl.ds(IMAGES, ROW)], xsem.at[h]) for h in range(2)]
    for x_copy in x_copies:
        x_copy.start()
    b_copy = pltpu.make_async_copy(bias_ref, bias_v, bsem)
    b_copy.start()

    barrier = pltpu.get_barrier_semaphore()
    pl.semaphore_signal(barrier, inc=1, device_id={"sp": up}, device_id_type=MESH)
    pl.semaphore_signal(barrier, inc=1, device_id={"sp": down}, device_id_type=MESH)
    pl.semaphore_signal(barrier, inc=1, device_id={"cp": other}, device_id_type=MESH)
    pl.semaphore_wait(barrier, 3)

    @pl.when(has_up)
    def _():
        x_send(0).start()

    @pl.when(has_down)
    def _():
        x_send(1).start()

    edge = jnp.zeros((4, IMAGES, CHUNK), jnp.bfloat16)
    zero = jnp.zeros((ROW, CHUNK), jnp.bfloat16)
    for w in (0, COLS + 1):
        for k in range(n2):
            xbuf[:, pl.ds(w * IMAGES, IMAGES), pl.ds(k * CHUNK, CHUNK)] = edge
        for j in range(n1):
            abuf[j, :, pl.ds(w * IMAGES, IMAGES), :] = edge

    def clear_row(r):
        for k in range(n2):
            xbuf[r, pl.ds(IMAGES, ROW), pl.ds(k * CHUNK, CHUNK)] = zero
        for j in range(n1):
            abuf[j, r, pl.ds(IMAGES, ROW), :] = zero

    @pl.when(jnp.logical_not(has_up))
    def _():
        clear_row(0)

    @pl.when(jnp.logical_not(has_down))
    def _():
        clear_row(3)

    b_copy.wait()
    for x_copy in x_copies:
        x_copy.wait()

    def group(slot, lhs, before_halo):
        total = None
        for i in range(3):
            if i == 1:
                before_halo()
            w_copy(w1_ref, 0, 0, slot, i).wait()
            for kx in range(3):
                part = jnp.dot(lhs(KY_ORDER[i], kx), wbuf[slot, i, kx], preferred_element_type=jnp.float32)
                total = part if total is None else total + part
        return total

    def x_lhs(ky, kx):
        return xbuf[pl.ds(ky, 2), pl.ds(kx * IMAGES, ROW), :].reshape(OWN, half_o)

    def wait_x_halo():
        @pl.when(has_up)
        def _():
            x_send(1).wait_recv()

        @pl.when(has_down)
        def _():
            x_send(0).wait_recv()

    def nothing():
        pass

    def conv1_step(j, carry):
        for side in range(2):
            g = 2 * j + side

            def before():
                if side == 0:
                    pl.when(j == 0)(wait_x_halo)

            if side == 0:
                slot = lax.rem(j, 2)

                @pl.when(j >= 2)
                def _():
                    part_send(slot, recv1.at[j], pr1_sem.at[j]).wait_send()

                send[slot] = group(lax.rem(g, slots), x_lhs, before)
                fetch(g + slots)
                part_send(slot, recv1.at[j], pr1_sem.at[j]).start()
            else:
                acc[...] = group(lax.rem(g, slots), x_lhs, before)
                fetch(g + slots)
                part_send(0, recv1.at[j], pr1_sem.at[j]).wait_recv()
                brow = c * (half_h // 128) + j * (CHUNK // 128)
                for h in range(2):
                    for q in range(CHUNK // 128):
                        rows, cols = pl.ds(h * ROW, ROW), pl.ds(q * 128, 128)
                        val = acc[rows, cols] + recv1[j, rows, cols] + bias_v[pl.ds(brow + q, 1), :]
                        abuf[j, 1 + h, pl.ds(IMAGES, ROW), cols] = jnp.maximum(val, 0.0).astype(jnp.bfloat16)

                @pl.when(has_up)
                def _():
                    halo_send(0, j).start()

                @pl.when(has_down)
                def _():
                    halo_send(1, j).start()
        return carry

    lax.fori_loop(0, n1, conv1_step, 0)

    per_kb = KBLOCK // CHUNK

    def conv2_chunk(m, first_pass, dst):
        dst[...] = jnp.zeros((OWN, CHUNK), jnp.float32)

        def kb_step(kb, carry):
            g = groups1 + m * kb2 + kb

            def a_lhs(ky, kx):
                return jnp.concatenate([abuf[kb * per_kb + d, pl.ds(ky, 2), pl.ds(kx * IMAGES, ROW), :].reshape(OWN, CHUNK)
                                        for d in range(per_kb)], axis=1)

            def wait_halo():
                for d in range(per_kb):
                    @pl.when(has_up)
                    def _():
                        halo_send(1, kb * per_kb + d).wait_recv()

                    @pl.when(has_down)
                    def _():
                        halo_send(0, kb * per_kb + d).wait_recv()

            part = group(lax.rem(g, slots), a_lhs, (lambda: pl.when(m == 0)(wait_halo)) if first_pass else nothing)
            dst[...] = dst[...] + part
            fetch(g + slots)
            return carry

        lax.fori_loop(0, kb2, kb_step, 0)

    def conv2_send(m, carry):
        slot = lax.rem(m, 2)
        part_send(slot, recv2.at[m], pr2_sem.at[m]).wait_send()
        conv2_chunk(m, True, send.at[slot])
        part_send(slot, recv2.at[m], pr2_sem.at[m]).start()
        return carry

    def conv2_own(m, carry):
        conv2_chunk(n2 + m, False, acc)
        part_send(0, recv2.at[m], pr2_sem.at[m]).wait_recv()
        cols = pl.ds(pl.multiple_of(m * CHUNK, CHUNK), CHUNK)
        for h in range(2):
            rows = pl.ds(h * ROW, ROW)
            val = xbuf[1 + h, pl.ds(IMAGES, ROW), cols].astype(jnp.float32) + (acc[rows, :] + recv2[m, rows, :])
            out_ref[rows, cols] = val.astype(jnp.bfloat16)
        return carry

    lax.fori_loop(0, n2, conv2_send, 0)
    lax.fori_loop(0, n2, conv2_own, 0)

    for slot in range(2):
        part_send(slot, recv2.at[slot], pr2_sem.at[slot]).wait_send()

    @pl.when(has_up)
    def _():
        x_send(0).wait_send()
        for j in range(n1):
            halo_send(0, j).wait_send()

    @pl.when(has_down)
    def _():
        x_send(1).wait_send()
        for j in range(n1):
            halo_send(1, j).wait_send()


def solution(mesh):
    sp_size = mesh.shape["sp"]
    act_spec = P("dp", "sp", None, "cp")
    kernel_spec = P(None, None, "cp", None)

    def local_block(x_tile, w_one, w_two, bias):
        half_o = x_tile.shape[3]
        chan, hidden = 2 * half_o, w_one.shape[3]
        half_h = hidden // 2
        n1, n2 = half_h // CHUNK, half_o // CHUNK
        x_rows = x_tile.transpose(1, 2, 0, 3).reshape(OWN, half_o)
        any_spec = pl.BlockSpec(memory_space=pl.ANY)
        dma = pltpu.SemaphoreType.DMA
        out = pl.pallas_call(
            functools.partial(resblock_kernel, sp_size, chan, hidden),
            out_shape=jax.ShapeDtypeStruct((OWN, half_o), jnp.bfloat16),
            in_specs=[any_spec] * 4,
            out_specs=pl.BlockSpec(memory_space=pltpu.VMEM),
            scratch_shapes=[
                pltpu.VMEM((4, ROW + 2 * IMAGES, half_o), jnp.bfloat16),
                pltpu.VMEM((n1, 4, ROW + 2 * IMAGES, CHUNK), jnp.bfloat16),
                pltpu.VMEM((4, 3, 3, KBLOCK, CHUNK), jnp.bfloat16),
                pltpu.VMEM((OWN, CHUNK), jnp.float32),
                pltpu.VMEM((2, OWN, CHUNK), jnp.float32),
                pltpu.VMEM((n1, OWN, CHUNK), jnp.float32),
                pltpu.VMEM((n2, OWN, CHUNK), jnp.float32),
                pltpu.VMEM((hidden // 128, 128), jnp.float32),
                dma((4, 3)), dma((2,)), dma, dma((2,)), dma((2,)), dma((2,)), dma((n1,)), dma((n2,)),
                dma((2, n1)), dma((2, n1)),
            ],
            compiler_params=pltpu.CompilerParams(
                collective_id=0, has_side_effects=True, vmem_limit_bytes=60 * 1024 * 1024),
        )(x_rows, w_one.reshape(9, half_o, hidden), w_two.reshape(9, half_h, chan), bias.reshape(hidden // 128, 128))
        return out.reshape(2, COLS, IMAGES, half_o).transpose(2, 0, 1, 3)

    return jax.shard_map(local_block, mesh=mesh, in_specs=(act_spec, kernel_spec, kernel_spec, P(None)), out_specs=act_spec, check_vma=False)
```

```python
import functools

import jax
import jax.numpy as jnp
from jax import lax
from jax.experimental import pallas as pl
from jax.experimental.pallas import tpu as pltpu
from jax.sharding import PartitionSpec as P

IMAGES = 16
COLS = 7
ROW = COLS * IMAGES
SIDE = ROW - IMAGES
OWN = 2 * ROW
CHUNK = 512
KBLOCK = 1024
SLOTS = 4
SOLO = 8
SHARED = 4
FIRST2 = SOLO + SHARED
LAST2 = FIRST2 + 4
GROUPS = LAST2 + 4
MESH = pl.DeviceIdType.MESH
TAPS = ((1, 0, 0, ROW), (0, 0, IMAGES, SIDE), (2, IMAGES, 0, SIDE))


def resblock_kernel(sp_size, half_o, half_h, x_ref, w1_ref, w2_ref, bias_ref, out_ref,
                    xbuf, abuf, asend, wbuf, stage, recv1, recv2, msend, mrecv, fin, bias_v,
                    wsem, xsem, bsem, xs_sem, xr_sem, ps_sem, pr1_sem, pr2_sem,
                    as_sem, ar_sem, os_sem, hs_sem, hr_sem, ms_sem, mr_sem):
    c = lax.axis_index("cp")
    s = lax.axis_index("sp")
    other = 1 - c
    p = lax.rem(s, 2)
    q = s // 2
    mate = s + 1 - 2 * p
    has_top = q > 0
    has_bot = q < sp_size // 2 - 1
    has_near = (s > 0) & (s < sp_size - 1)
    near_q = q + 2 * p - 1

    def w_copy(ref, kx, rows, cols, slot):
        return pltpu.make_async_copy(
            ref.at[:, kx, pl.ds(rows, KBLOCK), pl.ds(cols, CHUNK)], wbuf.at[slot, kx], wsem.at[slot, kx])

    def fetch(g):
        slot = lax.rem(g, SLOTS)

        @pl.when(g < FIRST2)
        def _():
            side = lax.rem(g, 2)
            unit = g // 2 + (g // SOLO) * 2 * p
            cols = (side * c + (1 - side) * other) * half_h + unit * CHUNK
            for kx, _, _, _ in TAPS:
                w_copy(w1_ref, kx, 0, pl.multiple_of(cols, CHUNK), slot).start()

        @pl.when((g >= FIRST2) & (g < GROUPS))
        def _():
            t = g - FIRST2
            m = t // 4
            r = lax.rem(t, 4)
            side = (1 - m) * lax.rem(r, 2) + m * (r // 2)
            kb = (1 - m) * (r // 2) + m * lax.rem(r, 2)
            cols = (side * c + (1 - side) * other) * half_o + m * CHUNK
            rows = kb * 2 * KBLOCK + p * KBLOCK
            for kx, _, _, _ in TAPS:
                w_copy(w2_ref, kx, pl.multiple_of(rows, KBLOCK), pl.multiple_of(cols, CHUNK), slot).start()

    def remote(src, dst, send_sem, recv_sem, device_id):
        return pltpu.make_async_remote_copy(src, dst, send_sem, recv_sem, device_id=device_id, device_id_type=MESH)

    def x_mate(i):
        row = 1 - p if i == 0 else p
        return remote(x_ref.at[pl.ds(row * ROW, ROW)], xbuf.at[1 + 2 * p + row], xs_sem.at[i], xr_sem.at[i], {"sp": mate})

    def x_outer(k):
        return remote(x_ref.at[pl.ds(p * ROW, ROW)], xbuf.at[5 * (1 - p)], xs_sem.at[2 + k], xr_sem.at[3 - p],
                      {"sp": 2 * near_q + k})

    def x_arrived(i):
        return remote(x_ref.at[pl.ds(0, ROW)], xbuf.at[0], xs_sem.at[0], xr_sem.at[i], {"sp": mate})

    def part_send(src, dst, ssem, rsem):
        return remote(src, dst, ssem, rsem, {"cp": other})

    def solo_part(u):
        return part_send(stage.at[lax.rem(u, 2), pl.ds(0, 2)], recv1.at[u], ps_sem.at[lax.rem(u, 2)], pr1_sem.at[u])

    def shared_part(t):
        return part_send(stage.at[t].reshape(2, 2, ROW, CHUNK), recv1.at[pl.ds(4 + 2 * t, 2)], ps_sem.at[t], pr1_sem.at[4 + t])

    def first2_part():
        return part_send(stage.at[0], recv2.at[0], ps_sem.at[0], pr2_sem.at[0])

    def last2_part(turn, r0):
        return part_send(stage.at[1, pl.ds(2 * turn, 2)], recv2.at[1, pl.ds(r0, 2)], ps_sem.at[1 + turn], pr2_sem.at[1 + turn])

    def unit_home(u):
        return lax.rem(u // 2, 2), (u // 4) * 2 + lax.rem(u, 2)

    def a_mate(u):
        _, j = unit_home(u)
        return remote(asend.at[u], abuf.at[j, pl.ds(1 + 2 * p, 2)], as_sem.at[u], ar_sem.at[j], {"sp": mate})

    def a_outer(u):
        k, j = unit_home(u)
        return remote(asend.at[u, p], abuf.at[j, 5 * (1 - p)], os_sem.at[u], hr_sem.at[1 - p, j], {"sp": 2 * near_q + k})

    def a_halo(i, t):
        return remote(abuf.at[2 + t, 1 + 3 * i], abuf.at[2 + t, 5 * (1 - i)], hs_sem.at[i, t], hr_sem.at[1 - i, 2 + t],
                      {"sp": lax.rem(s + sp_size + 4 * i - 2, sp_size)})

    def halo_arrived(i, j):
        return remote(abuf.at[0, 0], abuf.at[j, 5 * i], hs_sem.at[0, 0], hr_sem.at[i, j], {"sp": mate})

    def mate_sum(m):
        return remote(msend.at[m], mrecv.at[m], ms_sem.at[m], mr_sem.at[m], {"sp": mate})

    for g in range(SLOTS):
        fetch(jnp.int32(g))
    x_copies = [pltpu.make_async_copy(x_ref.at[pl.ds(h * ROW, ROW)], xbuf.at[1 + 2 * p + h], xsem.at[h]) for h in range(2)]
    for x_copy in x_copies:
        x_copy.start()
    b_copy = pltpu.make_async_copy(bias_ref, bias_v, bsem)
    b_copy.start()

    barrier = pltpu.get_barrier_semaphore()
    pl.semaphore_signal(barrier, inc=1, device_id={"cp": other}, device_id_type=MESH)
    for d in (sp_size - 2, sp_size - 1, 1, 2):
        pl.semaphore_signal(barrier, inc=1, device_id={"sp": lax.rem(s + d, sp_size)}, device_id_type=MESH)
    pl.semaphore_wait(barrier, 5)

    x_mate(0).start()

    @pl.when(has_near)
    def _():
        x_outer(1 - p).start()

    x_mate(1).start()

    @pl.when(has_near)
    def _():
        x_outer(p).start()

    zero = jnp.zeros((ROW, CHUNK), jnp.bfloat16)

    def clear_row(r):
        for k in range(half_o // CHUNK):
            xbuf[r, :, pl.ds(k * CHUNK, CHUNK)] = zero
        for j in range(4):
            abuf[j, r] = zero

    @pl.when(jnp.logical_not(has_top))
    def _():
        clear_row(0)

    @pl.when(jnp.logical_not(has_bot))
    def _():
        clear_row(5)

    b_copy.wait()
    for x_copy in x_copies:
        x_copy.wait()

    def group(slot, lhs, r0, nh, dst, d0, add, waiting=None):
        def wait():
            for kx, _, _, _ in TAPS:
                w_copy(w1_ref, kx, 0, 0, slot).wait()

        if waiting is None:
            wait()
        else:
            pl.when(waiting)(wait)
        for kx, src_col, dst_col, width in TAPS:
            total = None
            for ky in range(3):
                part = jnp.dot(lhs(r0 + ky, nh, src_col, width), wbuf[slot, kx, ky], preferred_element_type=jnp.float32)
                total = part if total is None else total + part
            total = total.reshape(nh, width, CHUNK)
            where = (pl.ds(d0, nh), pl.ds(dst_col, width), slice(None))
            if add or kx != 1:
                dst[where] = dst[where] + total
            else:
                dst[where] = total

    def x_lhs(r, nh, col, width):
        return xbuf[pl.ds(r, nh), pl.ds(col, width), :].reshape(nh * width, half_o)

    def bias_row(unit, n):
        return bias_v[pl.ds(c * (half_h // 128) + unit * (CHUNK // 128) + n, 1), :]

    def solo_step(g, carry):
        side = lax.rem(g, 2)
        u = g // 2
        dst = side * 2 + (1 - side) * lax.rem(u, 2)

        @pl.when((side == 0) & (u >= 2))
        def _():
            solo_part(u).wait_send()

        @pl.when(g == 0)
        def _():
            x_arrived(0).wait_recv()

            @pl.when(has_near)
            def _():
                x_arrived(2 + p).wait_recv()

        group(lax.rem(g, SLOTS), x_lhs, 2 * p, 2, stage.at[dst], 0, False)
        fetch(g + SLOTS)

        @pl.when(side == 0)
        def _():
            solo_part(u).start()

        @pl.when(side == 1)
        def _():
            solo_part(u).wait_recv()
            k, j = unit_home(u)
            for h in range(2):
                for n in range(CHUNK // 128):
                    cols = pl.ds(n * 128, 128)
                    val = stage[2, h, :, cols] + recv1[u, h, :, cols] + bias_row(u, n)
                    asend[u, h, :, cols] = jnp.maximum(val, 0.0).astype(jnp.bfloat16)

            @pl.when(k == p)
            def _():
                abuf[j, pl.ds(1 + 2 * p, 2)] = asend[u]

            @pl.when(k != p)
            def _():
                a_mate(u).start()

            @pl.when(has_near)
            def _():
                a_outer(u).start()
        return carry

    lax.fori_loop(0, SOLO, solo_step, 0)

    x_arrived(1).wait_recv()

    @pl.when(((p == 0) & has_bot) | ((p == 1) & has_top))
    def _():
        x_arrived(3 - p).wait_recv()

    def shared_step(i, carry):
        side = lax.rem(i, 2)
        t = i // 2
        dst = side * 2 + (1 - side) * t

        @pl.when(side == 0)
        def _():
            solo_part(t).wait_send()

        group(lax.rem(SOLO + i, SLOTS), x_lhs, 0, 4, stage.at[dst], 0, False)
        fetch(SOLO + i + SLOTS)

        @pl.when(side == 0)
        def _():
            shared_part(t).start()

        @pl.when(side == 1)
        def _():
            shared_part(t).wait_recv()
            for r in range(4):
                for n in range(CHUNK // 128):
                    cols = pl.ds(n * 128, 128)
                    val = stage[2, r, :, cols] + recv1[4 + 2 * t + r // 2, r % 2, :, cols] + bias_row(4 + 2 * p + t, n)
                    abuf[2 + t, 1 + r, :, cols] = jnp.maximum(val, 0.0).astype(jnp.bfloat16)

            @pl.when(has_top)
            def _():
                a_halo(0, t).start()

            @pl.when(has_bot)
            def _():
                a_halo(1, t).start()
        return carry

    lax.fori_loop(0, SHARED, shared_step, 0)

    def a_lhs(kb):
        def lhs(r, nh, col, width):
            return jnp.concatenate([abuf[2 * kb + d, pl.ds(r, nh), pl.ds(col, width), :].reshape(nh * width, CHUNK)
                                    for d in range(2)], axis=1)
        return lhs

    def first2_step(i, carry):
        side = lax.rem(i, 2)
        kb = i // 2
        dst = stage.at[side * 2]

        @pl.when(side == 0)
        def _():
            for d in range(2):
                j = 2 * kb + d

                @pl.when(kb == 0)
                def _():
                    remote(asend.at[0], abuf.at[j, pl.ds(1, 2)], as_sem.at[0], ar_sem.at[j], {"sp": mate}).wait_recv()

                @pl.when(has_top)
                def _():
                    halo_arrived(0, j).wait_recv()

                @pl.when(has_bot)
                def _():
                    halo_arrived(1, j).wait_recv()

        @pl.when(i == 0)
        def _():
            shared_part(0).wait_send()

        @pl.when(kb == 0)
        def _():
            dst[...] = jnp.zeros((4, ROW, CHUNK), jnp.float32)

        group(lax.rem(FIRST2 + i, SLOTS), a_lhs(kb), 0, 4, dst, 0, True)
        fetch(FIRST2 + i + SLOTS)

        @pl.when(i == 2)
        def _():
            first2_part().start()

        @pl.when(i == 3)
        def _():
            first2_part().wait_recv()
            msend[0] = stage[2, pl.ds(2 - 2 * p, 2)] + recv2[0, pl.ds(2 - 2 * p, 2)]
            mate_sum(0).start()
            fin[...] = stage[2, pl.ds(2 * p, 2)] + recv2[0, pl.ds(2 * p, 2)]
        return carry

    lax.fori_loop(0, 4, first2_step, 0)

    shared_part(1).wait_send()

    def last2_step(i, carry):
        turn = i // 4
        t = lax.rem(i, 4)
        side = t // 2
        kb = lax.rem(t, 2)
        r0 = 2 * lax.rem(p + 1 + turn, 2)
        dst = stage.at[1 + side]

        @pl.when(kb == 0)
        def _():
            dst[pl.ds(2 * turn, 2)] = jnp.zeros((2, ROW, CHUNK), jnp.float32)

        group(lax.rem(LAST2 + t, SLOTS), a_lhs(kb), r0, 2, dst, 2 * turn, True, turn == 0)

        @pl.when(t == 1)
        def _():
            last2_part(turn, r0).start()

        @pl.when(i == 3)
        def _():
            last2_part(0, r0).wait_recv()
            msend[1] = stage[2, pl.ds(0, 2)] + recv2[1, pl.ds(r0, 2)]
            mate_sum(1).start()

        def finish(m, value):
            for h in range(2):
                cols = pl.ds(m * CHUNK, CHUNK)
                total = value(h) + mrecv[m, h]
                out_ref[pl.ds(h * ROW, ROW), cols] = (xbuf[1 + 2 * p + h, :, cols].astype(jnp.float32) + total).astype(jnp.bfloat16)

        @pl.when(i == 5)
        def _():
            mate_sum(0).wait_recv()
            finish(0, lambda h: fin[h])

        @pl.when(i == 7)
        def _():
            last2_part(1, r0).wait_recv()
            mate_sum(1).wait_recv()
            finish(1, lambda h: stage[2, 2 + h] + recv2[1, r0 + h])
        return carry

    lax.fori_loop(0, 8, last2_step, 0)

    first2_part().wait_send()
    for turn in range(2):
        last2_part(turn, 0).wait_send()
    for m in range(2):
        mate_sum(m).wait_send()
        x_mate(m).wait_send()

    def drain_solo(u, carry):
        k, _ = unit_home(u)

        @pl.when(k != p)
        def _():
            a_mate(u).wait_send()

        @pl.when(has_near)
        def _():
            a_outer(u).wait_send()
        return carry

    lax.fori_loop(0, 4, drain_solo, 0)

    @pl.when(has_near)
    def _():
        for k in range(2):
            x_outer(k).wait_send()

    for i, exists in enumerate((has_top, has_bot)):
        @pl.when(exists)
        def _():
            for t in range(2):
                a_halo(i, t).wait_send()


def solution(mesh):
    sp_size = mesh.shape["sp"]
    act_spec = P("dp", "sp", None, "cp")
    kernel_spec = P(None, None, "cp", None)

    def local_block(x_tile, w_one, w_two, bias):
        half_o, half_h = x_tile.shape[3], w_two.shape[2]
        x_rows = x_tile.transpose(1, 2, 0, 3).reshape(OWN, half_o)
        any_spec = pl.BlockSpec(memory_space=pl.ANY)
        dma = pltpu.SemaphoreType.DMA
        f32, bf16 = jnp.float32, jnp.bfloat16
        out = pl.pallas_call(
            functools.partial(resblock_kernel, sp_size, half_o, half_h),
            out_shape=jax.ShapeDtypeStruct((OWN, half_o), bf16),
            in_specs=[any_spec] * 4,
            out_specs=pl.BlockSpec(memory_space=pltpu.VMEM),
            scratch_shapes=[
                pltpu.VMEM((6, ROW, half_o), bf16),
                pltpu.VMEM((4, 6, ROW, CHUNK), bf16),
                pltpu.VMEM((4, 2, ROW, CHUNK), bf16),
                pltpu.VMEM((SLOTS, 3, 3, KBLOCK, CHUNK), bf16),
                pltpu.VMEM((3, 4, ROW, CHUNK), f32),
                pltpu.VMEM((8, 2, ROW, CHUNK), f32),
                pltpu.VMEM((2, 4, ROW, CHUNK), f32),
                pltpu.VMEM((2, 2, ROW, CHUNK), f32),
                pltpu.VMEM((2, 2, ROW, CHUNK), f32),
                pltpu.VMEM((2, ROW, CHUNK), f32),
                pltpu.VMEM((2 * half_h // 128, 128), f32),
                dma((SLOTS, 3)), dma((2,)), dma, dma((4,)), dma((4,)), dma((3,)), dma((6,)), dma((3,)),
                dma((4,)), dma((2,)), dma((4,)), dma((2, 2)), dma((2, 4)), dma((2,)), dma((2,)),
            ],
            compiler_params=pltpu.CompilerParams(
                collective_id=0, has_side_effects=True, vmem_limit_bytes=58 * 1024 * 1024),
        )(x_rows, w_one, w_two, bias.reshape(2 * half_h // 128, 128))
        return out.reshape(2, COLS, IMAGES, half_o).transpose(2, 0, 1, 3)

    return jax.shard_map(local_block, mesh=mesh, in_specs=(act_spec, kernel_spec, kernel_spec, P(None)), out_specs=act_spec, check_vma=False)
```

```python
import functools

import jax
import jax.numpy as jnp
from jax import lax
from jax.experimental import pallas as pl
from jax.experimental.pallas import tpu as pltpu
from jax.sharding import PartitionSpec as P

IMAGES = 16
COLS = 7
ROW = COLS * IMAGES
SIDE = ROW - IMAGES
OWN = 2 * ROW
CHUNK = 512
KBLOCK = 1024
SLOTS = 4
SOLO = 8
SHARED = 4
SECOND = SOLO + SHARED
GROUPS = SECOND + 12
MESH = pl.DeviceIdType.MESH
TAPS = ((1, 0, 0, ROW), (0, 0, IMAGES, SIDE), (2, IMAGES, 0, SIDE))


def resblock_kernel(sp_size, half_o, half_h, x_ref, w1_ref, w2_ref, bias_ref, out_ref,
                    xbuf, abuf, asend, wbuf, stage, recv1, recv2, msend, mrecv, bias_v,
                    wsem, xsem, bsem, xs_sem, xr_sem, ps_sem, pr1_sem, po_sem, pr2_sem,
                    as_sem, ar_sem, os_sem, hs_sem, hr_sem, ms_sem, mr_sem):
    c = lax.axis_index("cp")
    s = lax.axis_index("sp")
    other = 1 - c
    p = lax.rem(s, 2)
    q = s // 2
    mate = s + 1 - 2 * p
    has_top = q > 0
    has_bot = q < sp_size // 2 - 1
    has_near = (s > 0) & (s < sp_size - 1)
    near_q = q + 2 * p - 1

    def w_copy(ref, kx, rows, cols, slot):
        return pltpu.make_async_copy(
            ref.at[:, kx, pl.ds(rows, KBLOCK), pl.ds(cols, CHUNK)], wbuf.at[slot, kx], wsem.at[slot, kx])

    def fetch(g):
        slot = lax.rem(g, SLOTS)

        @pl.when(g < SECOND)
        def _():
            side = lax.rem(g, 2)
            unit = g // 2 + (g // SOLO) * 2 * p
            cols = (side * c + (1 - side) * other) * half_h + unit * CHUNK
            for kx, _, _, _ in TAPS:
                w_copy(w1_ref, kx, 0, pl.multiple_of(cols, CHUNK), slot).start()

        @pl.when((g >= SECOND) & (g < GROUPS))
        def _():
            t = g - SECOND
            kb = lax.rem(t // 4, 2)
            m = lax.rem(t, 4) // 2
            side = lax.rem(t, 2)
            cols = (side * c + (1 - side) * other) * half_o + m * CHUNK
            rows = kb * 2 * KBLOCK + p * KBLOCK
            for kx, _, _, _ in TAPS:
                w_copy(w2_ref, kx, pl.multiple_of(rows, KBLOCK), pl.multiple_of(cols, CHUNK), slot).start()

    def remote(src, dst, send_sem, recv_sem, device_id):
        return pltpu.make_async_remote_copy(src, dst, send_sem, recv_sem, device_id=device_id, device_id_type=MESH)

    def x_mate(i):
        row = 1 - p if i == 0 else p
        return remote(x_ref.at[pl.ds(row * ROW, ROW)], xbuf.at[1 + 2 * p + row], xs_sem.at[i], xr_sem.at[i], {"sp": mate})

    def x_outer(k):
        return remote(x_ref.at[pl.ds(p * ROW, ROW)], xbuf.at[5 * (1 - p)], xs_sem.at[2 + k], xr_sem.at[3 - p],
                      {"sp": 2 * near_q + k})

    def x_arrived(i):
        return remote(x_ref.at[pl.ds(0, ROW)], xbuf.at[0], xs_sem.at[0], xr_sem.at[i], {"sp": mate})

    def part_send(src, dst, ssem, rsem):
        return remote(src, dst, ssem, rsem, {"cp": other})

    def solo_part(u):
        return part_send(stage.at[lax.rem(u, 2), pl.ds(0, 2)], recv1.at[u], ps_sem.at[lax.rem(u, 2)], pr1_sem.at[u])

    def shared_part(t):
        return part_send(stage.at[t].reshape(2, 2, ROW, CHUNK), recv1.at[pl.ds(4 + 2 * t, 2)], ps_sem.at[t], pr1_sem.at[4 + t])

    def out_part(turn, m, r0):
        return part_send(stage.at[m, pl.ds(2 * turn, 2)], recv2.at[m, pl.ds(r0, 2)], po_sem.at[turn, m], pr2_sem.at[turn, m])

    def unit_home(u):
        return lax.rem(u // 2, 2), (u // 4) * 2 + lax.rem(u, 2)

    def a_mate(u):
        _, j = unit_home(u)
        return remote(asend.at[u], abuf.at[j, pl.ds(1 + 2 * p, 2)], as_sem.at[u], ar_sem.at[j], {"sp": mate})

    def a_outer(u):
        k, j = unit_home(u)
        return remote(asend.at[u, p], abuf.at[j, 5 * (1 - p)], os_sem.at[u], hr_sem.at[1 - p, j], {"sp": 2 * near_q + k})

    def a_halo(i, t):
        return remote(abuf.at[2 + t, 1 + 3 * i], abuf.at[2 + t, 5 * (1 - i)], hs_sem.at[i, t], hr_sem.at[1 - i, 2 + t],
                      {"sp": lax.rem(s + sp_size + 4 * i - 2, sp_size)})

    def halo_arrived(i, j):
        return remote(abuf.at[0, 0], abuf.at[j, 5 * i], hs_sem.at[0, 0], hr_sem.at[i, j], {"sp": mate})

    def mate_sum(m):
        return remote(msend.at[m], mrecv.at[m], ms_sem.at[m], mr_sem.at[m], {"sp": mate})

    for g in range(SLOTS):
        fetch(jnp.int32(g))
    x_copies = [pltpu.make_async_copy(x_ref.at[pl.ds(h * ROW, ROW)], xbuf.at[1 + 2 * p + h], xsem.at[h]) for h in range(2)]
    for x_copy in x_copies:
        x_copy.start()
    b_copy = pltpu.make_async_copy(bias_ref, bias_v, bsem)
    b_copy.start()

    has_far = ((p == 0) & has_bot) | ((p == 1) & has_top)
    barrier = pltpu.get_barrier_semaphore()

    def greet(device_id):
        pl.semaphore_signal(barrier, inc=1, device_id=device_id, device_id_type=MESH)

    greet({"cp": other})
    greet({"sp": mate})

    @pl.when(has_near)
    def _():
        for k in range(2):
            greet({"sp": 2 * near_q + k})

    @pl.when(has_far)
    def _():
        greet({"sp": s + 2 - 4 * p})

    pl.semaphore_wait(barrier, 2 + 2 * has_near.astype(jnp.int32) + has_far.astype(jnp.int32))

    x_mate(0).start()

    @pl.when(has_near)
    def _():
        x_outer(1 - p).start()

    x_mate(1).start()

    @pl.when(has_near)
    def _():
        x_outer(p).start()

    zero = jnp.zeros((ROW, CHUNK), jnp.bfloat16)

    def clear_row(r):
        for k in range(half_o // CHUNK):
            xbuf[r, :, pl.ds(k * CHUNK, CHUNK)] = zero
        for j in range(4):
            abuf[j, r] = zero

    @pl.when(jnp.logical_not(has_top))
    def _():
        clear_row(0)

    @pl.when(jnp.logical_not(has_bot))
    def _():
        clear_row(5)

    b_copy.wait()
    for x_copy in x_copies:
        x_copy.wait()

    def group(slot, lhs, r0, nh, dst, d0, add, waiting=None):
        def wait():
            for kx, _, _, _ in TAPS:
                w_copy(w1_ref, kx, 0, 0, slot).wait()

        if waiting is None:
            wait()
        else:
            pl.when(waiting)(wait)
        for kx, src_col, dst_col, width in TAPS:
            total = None
            for ky in range(3):
                part = jnp.dot(lhs(r0 + ky, nh, src_col, width), wbuf[slot, kx, ky], preferred_element_type=jnp.float32)
                total = part if total is None else total + part
            total = total.reshape(nh, width, CHUNK)
            where = (pl.ds(d0, nh), pl.ds(dst_col, width), slice(None))
            if add or kx != 1:
                dst[where] = dst[where] + total
            else:
                dst[where] = total

    def x_lhs(r, nh, col, width):
        return xbuf[pl.ds(r, nh), pl.ds(col, width), :].reshape(nh * width, half_o)

    def bias_row(unit, n):
        return bias_v[pl.ds(c * (half_h // 128) + unit * (CHUNK // 128) + n, 1), :]

    def solo_step(g, carry):
        side = lax.rem(g, 2)
        u = g // 2
        dst = side * 2 + (1 - side) * lax.rem(u, 2)

        @pl.when((side == 0) & (u >= 2))
        def _():
            solo_part(u).wait_send()

        @pl.when(g == 0)
        def _():
            x_arrived(0).wait_recv()

            @pl.when(has_near)
            def _():
                x_arrived(2 + p).wait_recv()

        group(lax.rem(g, SLOTS), x_lhs, 2 * p, 2, stage.at[dst], 0, False)
        fetch(g + SLOTS)

        @pl.when(side == 0)
        def _():
            solo_part(u).start()

        @pl.when(side == 1)
        def _():
            solo_part(u).wait_recv()
            k, j = unit_home(u)
            for h in range(2):
                for n in range(CHUNK // 128):
                    cols = pl.ds(n * 128, 128)
                    val = stage[2, h, :, cols] + recv1[u, h, :, cols] + bias_row(u, n)
                    asend[u, h, :, cols] = jnp.maximum(val, 0.0).astype(jnp.bfloat16)

            @pl.when(k == p)
            def _():
                abuf[j, pl.ds(1 + 2 * p, 2)] = asend[u]

            @pl.when(k != p)
            def _():
                a_mate(u).start()

            @pl.when(has_near)
            def _():
                a_outer(u).start()
        return carry

    lax.fori_loop(0, SOLO, solo_step, 0)

    x_arrived(1).wait_recv()

    @pl.when(has_far)
    def _():
        x_arrived(3 - p).wait_recv()

    def shared_step(i, carry):
        side = lax.rem(i, 2)
        t = i // 2
        dst = side * 2 + (1 - side) * t

        @pl.when(side == 0)
        def _():
            solo_part(t).wait_send()

        group(lax.rem(SOLO + i, SLOTS), x_lhs, 0, 4, stage.at[dst], 0, False)
        fetch(SOLO + i + SLOTS)

        @pl.when(side == 0)
        def _():
            shared_part(t).start()

        @pl.when(side == 1)
        def _():
            shared_part(t).wait_recv()
            for r in range(4):
                for n in range(CHUNK // 128):
                    cols = pl.ds(n * 128, 128)
                    val = stage[2, r, :, cols] + recv1[4 + 2 * t + r // 2, r % 2, :, cols] + bias_row(4 + 2 * p + t, n)
                    abuf[2 + t, 1 + r, :, cols] = jnp.maximum(val, 0.0).astype(jnp.bfloat16)

            @pl.when(has_top)
            def _():
                a_halo(0, t).start()

            @pl.when(has_bot)
            def _():
                a_halo(1, t).start()
        return carry

    lax.fori_loop(0, SHARED, shared_step, 0)

    def a_lhs(kb):
        def lhs(r, nh, col, width):
            return jnp.concatenate([abuf[2 * kb + d, pl.ds(r, nh), pl.ds(col, width), :].reshape(nh * width, CHUNK)
                                    for d in range(2)], axis=1)
        return lhs

    def wait_a(kb):
        for d in range(2):
            j = 2 * kb + d
            if kb == 0:
                remote(asend.at[0], abuf.at[j, pl.ds(1, 2)], as_sem.at[0], ar_sem.at[j], {"sp": mate}).wait_recv()

            @pl.when(has_top)
            def _():
                halo_arrived(0, j).wait_recv()

            @pl.when(has_bot)
            def _():
                halo_arrived(1, j).wait_recv()

    for t in range(2):
        shared_part(t).wait_send()
    stage[...] = jnp.zeros((4, 4, ROW, CHUNK), jnp.float32)

    def second_step(i, carry):
        turn = i // 8
        t = lax.rem(i, 4)
        last = lax.rem(i // 4, 2)
        kb = lax.rem(turn + last, 2)
        m = t // 2
        side = lax.rem(t, 2)
        r0 = 2 * lax.rem(p + 1 + turn, 2)
        g = SECOND + i - 4 * turn

        for k in range(2):
            @pl.when(i == 4 * k)
            def _():
                wait_a(k)

        group(lax.rem(g, SLOTS), a_lhs(kb), r0, 2, stage.at[2 * side + m], 2 * turn, True, i // 4 != 2)

        @pl.when(i // 4 != 1)
        def _():
            fetch(g + SLOTS)

        @pl.when((last == 1) & (side == 0))
        def _():
            out_part(turn, m, r0).start()

        @pl.when((last == 1) & (side == 1))
        def _():
            out_part(turn, m, r0).wait_recv()

            @pl.when(turn == 0)
            def _():
                msend[m] = stage[2 + m, pl.ds(0, 2)] + recv2[m, pl.ds(r0, 2)]
                mate_sum(m).start()

            @pl.when(turn == 1)
            def _():
                mate_sum(m).wait_recv()
                cols = pl.ds(pl.multiple_of(m * CHUNK, CHUNK), CHUNK)
                for h in range(2):
                    total = stage[2 + m, 2 + h] + recv2[m, r0 + h] + mrecv[m, h]
                    out_ref[pl.ds(h * ROW, ROW), cols] = (xbuf[1 + 2 * p + h, :, cols].astype(jnp.float32) + total).astype(jnp.bfloat16)
        return carry

    lax.fori_loop(0, 16, second_step, 0)

    for m in range(2):
        for turn in range(2):
            out_part(turn, m, 0).wait_send()
        mate_sum(m).wait_send()
        x_mate(m).wait_send()

    def drain_solo(u, carry):
        k, _ = unit_home(u)

        @pl.when(k != p)
        def _():
            a_mate(u).wait_send()

        @pl.when(has_near)
        def _():
            a_outer(u).wait_send()
        return carry

    lax.fori_loop(0, 4, drain_solo, 0)

    @pl.when(has_near)
    def _():
        for k in range(2):
            x_outer(k).wait_send()

    for i, exists in enumerate((has_top, has_bot)):
        @pl.when(exists)
        def _():
            for t in range(2):
                a_halo(i, t).wait_send()


def solution(mesh):
    sp_size = mesh.shape["sp"]
    act_spec = P("dp", "sp", None, "cp")
    kernel_spec = P(None, None, "cp", None)

    def local_block(x_tile, w_one, w_two, bias):
        half_o, half_h = x_tile.shape[3], w_two.shape[2]
        x_rows = x_tile.transpose(1, 2, 0, 3).reshape(OWN, half_o)
        any_spec = pl.BlockSpec(memory_space=pl.ANY)
        dma = pltpu.SemaphoreType.DMA
        f32, bf16 = jnp.float32, jnp.bfloat16
        out = pl.pallas_call(
            functools.partial(resblock_kernel, sp_size, half_o, half_h),
            out_shape=jax.ShapeDtypeStruct((OWN, half_o), bf16),
            in_specs=[any_spec] * 4,
            out_specs=pl.BlockSpec(memory_space=pltpu.VMEM),
            scratch_shapes=[
                pltpu.VMEM((6, ROW, half_o), bf16),
                pltpu.VMEM((4, 6, ROW, CHUNK), bf16),
                pltpu.VMEM((4, 2, ROW, CHUNK), bf16),
                pltpu.VMEM((SLOTS, 3, 3, KBLOCK, CHUNK), bf16),
                pltpu.VMEM((4, 4, ROW, CHUNK), f32),
                pltpu.VMEM((8, 2, ROW, CHUNK), f32),
                pltpu.VMEM((2, 4, ROW, CHUNK), f32),
                pltpu.VMEM((2, 2, ROW, CHUNK), f32),
                pltpu.VMEM((2, 2, ROW, CHUNK), f32),
                pltpu.VMEM((2 * half_h // 128, 128), f32),
                dma((SLOTS, 3)), dma((2,)), dma, dma((4,)), dma((4,)), dma((2,)), dma((6,)), dma((2, 2)), dma((2, 2)),
                dma((4,)), dma((2,)), dma((4,)), dma((2, 2)), dma((2, 4)), dma((2,)), dma((2,)),
            ],
            compiler_params=pltpu.CompilerParams(
                collective_id=0, has_side_effects=True, vmem_limit_bytes=53 * 1024 * 1024),
        )(x_rows, w_one, w_two, bias.reshape(2 * half_h // 128, 128))
        return out.reshape(2, COLS, IMAGES, half_o).transpose(2, 0, 1, 3)

    return jax.shard_map(local_block, mesh=mesh, in_specs=(act_spec, kernel_spec, kernel_spec, P(None)), out_specs=act_spec, check_vma=False)
```

```python
import functools

import jax
import jax.numpy as jnp
from jax import lax
from jax.experimental import pallas as pl
from jax.experimental.pallas import tpu as pltpu
from jax.sharding import PartitionSpec as P

IMAGES = 16
COLS = 7
ROW = COLS * IMAGES
SIDE = ROW - IMAGES
OWN = 2 * ROW
CHUNK = 512
KBLOCK = 1024
SLOTS = 4
SOLO = 4
SHARED = 6
UNITS = 4
SECOND = SOLO + SHARED
GROUPS = SECOND + 12
MESH = pl.DeviceIdType.MESH
TAPS = ((1, 0, 0, ROW), (0, 0, IMAGES, SIDE), (2, IMAGES, 0, SIDE))


def resblock_kernel(sp_size, half_o, half_h, x_ref, w1_ref, w2_ref, bias_ref, out_ref,
                    xbuf, abuf, asend, wbuf, stage, recv1, recv2, msend, mrecv, bias_v,
                    wsem, xsem, bsem, xs_sem, xr_sem, ps_sem, pr1_sem, po_sem, pr2_sem,
                    as_sem, ar_sem, os_sem, hs_sem, hr_sem, ms_sem, mr_sem):
    c = lax.axis_index("cp")
    s = lax.axis_index("sp")
    other = 1 - c
    p = lax.rem(s, 2)
    q = s // 2
    mate = s + 1 - 2 * p
    has_top = q > 0
    has_bot = q < sp_size // 2 - 1
    has_near = (s > 0) & (s < sp_size - 1)
    near_q = q + 2 * p - 1

    def w_copy(ref, kx, rows, cols, slot):
        return pltpu.make_async_copy(
            ref.at[:, kx, pl.ds(rows, KBLOCK), pl.ds(cols, CHUNK)], wbuf.at[slot, kx], wsem.at[slot, kx])

    def fetch(g):
        slot = lax.rem(g, SLOTS)

        @pl.when(g < SECOND)
        def _():
            side = lax.rem(g, 2)
            u = g // 2
            shared = (g + SECOND - SOLO) // SECOND
            unit = (1 - shared) * (UNITS * lax.rem(u, 2) + u // 2) + shared * (UNITS * p + u - SOLO // 4)
            cols = (side * c + (1 - side) * other) * half_h + unit * CHUNK
            for kx, _, _, _ in TAPS:
                w_copy(w1_ref, kx, 0, pl.multiple_of(cols, CHUNK), slot).start()

        @pl.when((g >= SECOND) & (g < GROUPS))
        def _():
            t = g - SECOND
            kb = lax.rem(t // 4, 2)
            m = lax.rem(t, 4) // 2
            side = lax.rem(t, 2)
            cols = (side * c + (1 - side) * other) * half_o + m * CHUNK
            rows = p * 2 * KBLOCK + kb * KBLOCK
            for kx, _, _, _ in TAPS:
                w_copy(w2_ref, kx, pl.multiple_of(rows, KBLOCK), pl.multiple_of(cols, CHUNK), slot).start()

    def remote(src, dst, send_sem, recv_sem, device_id):
        return pltpu.make_async_remote_copy(src, dst, send_sem, recv_sem, device_id=device_id, device_id_type=MESH)

    def x_mate(i):
        row = 1 - p if i == 0 else p
        return remote(x_ref.at[pl.ds(row * ROW, ROW)], xbuf.at[1 + 2 * p + row], xs_sem.at[i], xr_sem.at[i], {"sp": mate})

    def x_outer(k):
        return remote(x_ref.at[pl.ds(p * ROW, ROW)], xbuf.at[5 * (1 - p)], xs_sem.at[2 + k], xr_sem.at[3 - p],
                      {"sp": 2 * near_q + k})

    def x_arrived(i):
        return remote(x_ref.at[pl.ds(0, ROW)], xbuf.at[0], xs_sem.at[0], xr_sem.at[i], {"sp": mate})

    def part_send(src, dst, ssem, rsem):
        return remote(src, dst, ssem, rsem, {"cp": other})

    def solo_part(u):
        return part_send(stage.at[lax.rem(u, 2), pl.ds(0, 2)], recv1.at[u], ps_sem.at[lax.rem(u, 2)], pr1_sem.at[u])

    def shared_part(t):
        slot = lax.rem(t, 2)
        return part_send(stage.at[slot].reshape(2, 2, ROW, CHUNK), recv1.at[pl.ds(SOLO // 2 + 2 * t, 2)],
                         ps_sem.at[slot], pr1_sem.at[SOLO // 2 + t])

    def out_part(turn, m, r0):
        return part_send(stage.at[m, pl.ds(2 * turn, 2)], recv2.at[m, pl.ds(r0, 2)], po_sem.at[turn, m], pr2_sem.at[turn, m])

    def unit_home(u):
        return lax.rem(u, 2), u // 2

    def a_mate(u):
        _, j = unit_home(u)
        return remote(asend.at[u], abuf.at[j, pl.ds(1 + 2 * p, 2)], as_sem.at[u], ar_sem.at[j], {"sp": mate})

    def a_outer(u):
        k, j = unit_home(u)
        return remote(asend.at[u, p], abuf.at[j, 5 * (1 - p)], os_sem.at[u], hr_sem.at[1 - p, j], {"sp": 2 * near_q + k})

    def a_halo(i, t):
        j = SOLO // 4 + t
        return remote(abuf.at[j, 1 + 3 * i], abuf.at[j, 5 * (1 - i)], hs_sem.at[i, t], hr_sem.at[1 - i, j],
                      {"sp": lax.rem(s + sp_size + 4 * i - 2, sp_size)})

    def halo_arrived(i, j):
        return remote(abuf.at[0, 0], abuf.at[j, 5 * i], hs_sem.at[0, 0], hr_sem.at[i, j], {"sp": mate})

    def mate_sum(m):
        return remote(msend.at[m], mrecv.at[m], ms_sem.at[m], mr_sem.at[m], {"sp": mate})

    for g in range(SLOTS):
        fetch(jnp.int32(g))
    x_copies = [pltpu.make_async_copy(x_ref.at[pl.ds(h * ROW, ROW)], xbuf.at[1 + 2 * p + h], xsem.at[h]) for h in range(2)]
    for x_copy in x_copies:
        x_copy.start()
    b_copy = pltpu.make_async_copy(bias_ref, bias_v, bsem)
    b_copy.start()

    has_far = ((p == 0) & has_bot) | ((p == 1) & has_top)
    barrier = pltpu.get_barrier_semaphore()

    def greet(device_id):
        pl.semaphore_signal(barrier, inc=1, device_id=device_id, device_id_type=MESH)

    greet({"cp": other})
    greet({"sp": mate})

    @pl.when(has_near)
    def _():
        for k in range(2):
            greet({"sp": 2 * near_q + k})

    @pl.when(has_far)
    def _():
        greet({"sp": s + 2 - 4 * p})

    pl.semaphore_wait(barrier, 2 + 2 * has_near.astype(jnp.int32) + has_far.astype(jnp.int32))

    x_mate(0).start()

    @pl.when(has_near)
    def _():
        x_outer(1 - p).start()

    x_mate(1).start()

    @pl.when(has_near)
    def _():
        x_outer(p).start()

    zero = jnp.zeros((ROW, CHUNK), jnp.bfloat16)

    def clear_row(r):
        for k in range(half_o // CHUNK):
            xbuf[r, :, pl.ds(k * CHUNK, CHUNK)] = zero
        for j in range(4):
            abuf[j, r] = zero

    @pl.when(jnp.logical_not(has_top))
    def _():
        clear_row(0)

    @pl.when(jnp.logical_not(has_bot))
    def _():
        clear_row(5)

    b_copy.wait()
    for x_copy in x_copies:
        x_copy.wait()

    def group(slot, lhs, r0, nh, dst, d0, add, waiting=None):
        def wait():
            for kx, _, _, _ in TAPS:
                w_copy(w1_ref, kx, 0, 0, slot).wait()

        if waiting is None:
            wait()
        else:
            pl.when(waiting)(wait)
        for kx, src_col, dst_col, width in TAPS:
            total = None
            for ky in range(3):
                part = jnp.dot(lhs(r0 + ky, nh, src_col, width), wbuf[slot, kx, ky], preferred_element_type=jnp.float32)
                total = part if total is None else total + part
            total = total.reshape(nh, width, CHUNK)
            where = (pl.ds(d0, nh), pl.ds(dst_col, width), slice(None))
            if add or kx != 1:
                dst[where] = dst[where] + total
            else:
                dst[where] = total

    def x_lhs(r, nh, col, width):
        return xbuf[pl.ds(r, nh), pl.ds(col, width), :].reshape(nh * width, half_o)

    def bias_row(unit, n):
        return bias_v[pl.ds(c * (half_h // 128) + unit * (CHUNK // 128) + n, 1), :]

    def solo_step(g, carry):
        side = lax.rem(g, 2)
        u = g // 2
        dst = side * 2 + (1 - side) * u

        @pl.when(g == 0)
        def _():
            x_arrived(0).wait_recv()

            @pl.when(has_near)
            def _():
                x_arrived(2 + p).wait_recv()

        group(lax.rem(g, SLOTS), x_lhs, 2 * p, 2, stage.at[dst], 0, False)
        fetch(g + SLOTS)

        @pl.when(side == 0)
        def _():
            solo_part(u).start()

        @pl.when(side == 1)
        def _():
            solo_part(u).wait_recv()
            k, j = unit_home(u)
            for h in range(2):
                for n in range(CHUNK // 128):
                    cols = pl.ds(n * 128, 128)
                    val = stage[2, h, :, cols] + recv1[u, h, :, cols] + bias_row(UNITS * k + j, n)
                    asend[u, h, :, cols] = jnp.maximum(val, 0.0).astype(jnp.bfloat16)

            @pl.when(k == p)
            def _():
                abuf[j, pl.ds(1 + 2 * p, 2)] = asend[u]

            @pl.when(k != p)
            def _():
                a_mate(u).start()

            @pl.when(has_near)
            def _():
                a_outer(u).start()
        return carry

    lax.fori_loop(0, SOLO, solo_step, 0)

    x_arrived(1).wait_recv()

    @pl.when(has_far)
    def _():
        x_arrived(3 - p).wait_recv()

    def shared_step(i, carry):
        side = lax.rem(i, 2)
        t = i // 2
        dst = side * 2 + (1 - side) * lax.rem(t, 2)

        @pl.when((side == 0) & (t < 2))
        def _():
            solo_part(t).wait_send()

        @pl.when((side == 0) & (t >= 2))
        def _():
            shared_part(t).wait_send()

        group(lax.rem(SOLO + i, SLOTS), x_lhs, 0, 4, stage.at[dst], 0, False)
        fetch(SOLO + i + SLOTS)

        @pl.when(side == 0)
        def _():
            shared_part(t).start()

        @pl.when(side == 1)
        def _():
            shared_part(t).wait_recv()
            for r in range(4):
                for n in range(CHUNK // 128):
                    cols = pl.ds(n * 128, 128)
                    val = stage[2, r, :, cols] + recv1[SOLO // 2 + 2 * t + r // 2, r % 2, :, cols] + bias_row(UNITS * p + SOLO // 4 + t, n)
                    abuf[SOLO // 4 + t, 1 + r, :, cols] = jnp.maximum(val, 0.0).astype(jnp.bfloat16)

            @pl.when(has_top)
            def _():
                a_halo(0, t).start()

            @pl.when(has_bot)
            def _():
                a_halo(1, t).start()
        return carry

    lax.fori_loop(0, SHARED, shared_step, 0)

    def a_lhs(kb):
        def lhs(r, nh, col, width):
            return jnp.concatenate([abuf[2 * kb + d, pl.ds(r, nh), pl.ds(col, width), :].reshape(nh * width, CHUNK)
                                    for d in range(2)], axis=1)
        return lhs

    def wait_a(kb):
        for d in range(2):
            j = 2 * kb + d
            if j < SOLO // 4:
                remote(asend.at[0], abuf.at[j, pl.ds(1, 2)], as_sem.at[0], ar_sem.at[j], {"sp": mate}).wait_recv()

            @pl.when(has_top)
            def _():
                halo_arrived(0, j).wait_recv()

            @pl.when(has_bot)
            def _():
                halo_arrived(1, j).wait_recv()

    for t in range(SHARED // 2 - 2, SHARED // 2):
        shared_part(jnp.int32(t)).wait_send()
    stage[...] = jnp.zeros((4, 4, ROW, CHUNK), jnp.float32)

    def second_step(i, carry):
        turn = i // 8
        t = lax.rem(i, 4)
        last = lax.rem(i // 4, 2)
        kb = lax.rem(turn + last, 2)
        m = t // 2
        side = lax.rem(t, 2)
        r0 = 2 * lax.rem(p + 1 + turn, 2)
        g = SECOND + i - 4 * turn

        for k in range(2):
            @pl.when(i == 4 * k)
            def _():
                wait_a(k)

        group(lax.rem(g, SLOTS), a_lhs(kb), r0, 2, stage.at[2 * side + m], 2 * turn, True, i // 4 != 2)

        @pl.when(i // 4 != 1)
        def _():
            fetch(g + SLOTS)

        @pl.when((last == 1) & (side == 0))
        def _():
            out_part(turn, m, r0).start()

        @pl.when((last == 1) & (side == 1))
        def _():
            out_part(turn, m, r0).wait_recv()

            @pl.when(turn == 0)
            def _():
                msend[m] = stage[2 + m, pl.ds(0, 2)] + recv2[m, pl.ds(r0, 2)]
                mate_sum(m).start()

            @pl.when(turn == 1)
            def _():
                mate_sum(m).wait_recv()
                cols = pl.ds(pl.multiple_of(m * CHUNK, CHUNK), CHUNK)
                for h in range(2):
                    total = stage[2 + m, 2 + h] + recv2[m, r0 + h] + mrecv[m, h]
                    out_ref[pl.ds(h * ROW, ROW), cols] = (xbuf[1 + 2 * p + h, :, cols].astype(jnp.float32) + total).astype(jnp.bfloat16)
        return carry

    lax.fori_loop(0, 16, second_step, 0)

    for m in range(2):
        for turn in range(2):
            out_part(turn, m, 0).wait_send()
        mate_sum(m).wait_send()
        x_mate(m).wait_send()

    def drain_solo(u, carry):
        k, _ = unit_home(u)

        @pl.when(k != p)
        def _():
            a_mate(u).wait_send()

        @pl.when(has_near)
        def _():
            a_outer(u).wait_send()
        return carry

    lax.fori_loop(0, SOLO // 2, drain_solo, 0)

    @pl.when(has_near)
    def _():
        for k in range(2):
            x_outer(k).wait_send()

    for i, exists in enumerate((has_top, has_bot)):
        @pl.when(exists)
        def _():
            for t in range(SHARED // 2):
                a_halo(i, t).wait_send()


def solution(mesh):
    sp_size = mesh.shape["sp"]
    act_spec = P("dp", "sp", None, "cp")
    kernel_spec = P(None, None, "cp", None)

    def local_block(x_tile, w_one, w_two, bias):
        half_o, half_h = x_tile.shape[3], w_two.shape[2]
        x_rows = x_tile.transpose(1, 2, 0, 3).reshape(OWN, half_o)
        any_spec = pl.BlockSpec(memory_space=pl.ANY)
        dma = pltpu.SemaphoreType.DMA
        f32, bf16 = jnp.float32, jnp.bfloat16
        out = pl.pallas_call(
            functools.partial(resblock_kernel, sp_size, half_o, half_h),
            out_shape=jax.ShapeDtypeStruct((OWN, half_o), bf16),
            in_specs=[any_spec] * 4,
            out_specs=pl.BlockSpec(memory_space=pltpu.VMEM),
            scratch_shapes=[
                pltpu.VMEM((6, ROW, half_o), bf16),
                pltpu.VMEM((4, 6, ROW, CHUNK), bf16),
                pltpu.VMEM((SOLO // 2, 2, ROW, CHUNK), bf16),
                pltpu.VMEM((SLOTS, 3, 3, KBLOCK, CHUNK), bf16),
                pltpu.VMEM((4, 4, ROW, CHUNK), f32),
                pltpu.VMEM((8, 2, ROW, CHUNK), f32),
                pltpu.VMEM((2, 4, ROW, CHUNK), f32),
                pltpu.VMEM((2, 2, ROW, CHUNK), f32),
                pltpu.VMEM((2, 2, ROW, CHUNK), f32),
                pltpu.VMEM((2 * half_h // 128, 128), f32),
                dma((SLOTS, 3)), dma((2,)), dma, dma((4,)), dma((4,)), dma((2,)), dma(((SOLO + SHARED) // 2,)), dma((2, 2)), dma((2, 2)),
                dma((SOLO // 2,)), dma((SOLO // 4,)), dma((SOLO // 2,)), dma((2, SHARED // 2)), dma((2, 4)), dma((2,)), dma((2,)),
            ],
            compiler_params=pltpu.CompilerParams(
                collective_id=0, has_side_effects=True, vmem_limit_bytes=53 * 1024 * 1024),
        )(x_rows, w_one, w_two, bias.reshape(2 * half_h // 128, 128))
        return out.reshape(2, COLS, IMAGES, half_o).transpose(2, 0, 1, 3)

    return jax.shard_map(local_block, mesh=mesh, in_specs=(act_spec, kernel_spec, kernel_spec, P(None)), out_specs=act_spec, check_vma=False)
```

```python
import functools

import jax
import jax.numpy as jnp
from jax import lax
from jax.experimental import pallas as pl
from jax.experimental.pallas import tpu as pltpu
from jax.sharding import PartitionSpec as P

IMAGES = 16
COLS = 7
ROW = COLS * IMAGES
SIDE = ROW - IMAGES
OWN = 2 * ROW
CHUNK = 512
KBLOCK = 1024
SLOTS = 4
SOLO = 4
SHARED = 6
UNITS = 4
SECOND = SOLO + SHARED
GROUPS = SECOND + 12
MESH = pl.DeviceIdType.MESH
TAPS = ((1, 0, 0, ROW), (0, 0, IMAGES, SIDE), (2, IMAGES, 0, SIDE))


def resblock_kernel(sp_size, half_o, half_h, x_ref, w1_ref, w2_ref, bias_ref, out_ref,
                    xbuf, abuf, asend, wbuf, stage, recv1, recv2, msend, mrecv, bias_v,
                    wsem, xsem, bsem, xs_sem, xr_sem, ps_sem, pr1_sem, po_sem, pr2_sem,
                    as_sem, ar_sem, os_sem, hs_sem, hr_sem, ms_sem, mr_sem):
    c = lax.axis_index("cp")
    s = lax.axis_index("sp")
    other = 1 - c
    p = lax.rem(s, 2)
    q = s // 2
    mate = s + 1 - 2 * p
    has_top = q > 0
    has_bot = q < sp_size // 2 - 1
    has_near = (s > 0) & (s < sp_size - 1)
    near_q = q + 2 * p - 1
    share = lax.rem(p + q, 2)

    def w_copy(ref, kx, rows, cols, slot):
        return pltpu.make_async_copy(
            ref.at[:, kx, pl.ds(rows, KBLOCK), pl.ds(cols, CHUNK)], wbuf.at[slot, kx], wsem.at[slot, kx])

    def fetch(g):
        slot = lax.rem(g, SLOTS)

        @pl.when(g < SECOND)
        def _():
            side = lax.rem(g, 2)
            u = g // 2
            shared = (g + SECOND - SOLO) // SECOND
            unit = (1 - shared) * (UNITS * lax.rem(u, 2) + u // 2) + shared * (UNITS * share + u - SOLO // 4)
            cols = (side * c + (1 - side) * other) * half_h + unit * CHUNK
            for kx, _, _, _ in TAPS:
                w_copy(w1_ref, kx, 0, pl.multiple_of(cols, CHUNK), slot).start()

        @pl.when((g >= SECOND) & (g < GROUPS))
        def _():
            t = g - SECOND
            kb = lax.rem(t // 4, 2)
            m = lax.rem(t, 4) // 2
            side = lax.rem(t, 2)
            cols = (side * c + (1 - side) * other) * half_o + m * CHUNK
            rows = share * 2 * KBLOCK + kb * KBLOCK
            for kx, _, _, _ in TAPS:
                w_copy(w2_ref, kx, pl.multiple_of(rows, KBLOCK), pl.multiple_of(cols, CHUNK), slot).start()

    def remote(src, dst, send_sem, recv_sem, device_id):
        return pltpu.make_async_remote_copy(src, dst, send_sem, recv_sem, device_id=device_id, device_id_type=MESH)

    def x_mate(i):
        row = 1 - p if i == 0 else p
        return remote(x_ref.at[pl.ds(row * ROW, ROW)], xbuf.at[1 + 2 * p + row], xs_sem.at[i], xr_sem.at[i], {"sp": mate})

    def x_outer():
        return remote(x_ref.at[pl.ds(p * ROW, ROW)], xbuf.at[5 * (1 - p)], xs_sem.at[2], xr_sem.at[3 - p],
                      {"sp": 2 * near_q + 1 - p})

    def x_forward():
        return remote(xbuf.at[5 * p], xbuf.at[5 * p], xs_sem.at[3], xr_sem.at[2 + p], {"sp": mate})

    def x_arrived(i):
        return remote(x_ref.at[pl.ds(0, ROW)], xbuf.at[0], xs_sem.at[0], xr_sem.at[i], {"sp": mate})

    def part_send(src, dst, ssem, rsem):
        return remote(src, dst, ssem, rsem, {"cp": other})

    def solo_part(u):
        return part_send(stage.at[lax.rem(u, 2), pl.ds(0, 2)], recv1.at[u], ps_sem.at[lax.rem(u, 2)], pr1_sem.at[u])

    def shared_part(t):
        slot = lax.rem(t, 2)
        return part_send(stage.at[slot].reshape(2, 2, ROW, CHUNK), recv1.at[pl.ds(SOLO // 2 + 2 * t, 2)],
                         ps_sem.at[slot], pr1_sem.at[SOLO // 2 + t])

    def out_part(turn, m, r0):
        return part_send(stage.at[m, pl.ds(2 * turn, 2)], recv2.at[m, pl.ds(r0, 2)], po_sem.at[turn, m], pr2_sem.at[turn, m])

    def unit_home(u):
        return lax.rem(u, 2), u // 2

    def a_mate(u):
        _, j = unit_home(u)
        return remote(asend.at[u], abuf.at[j, pl.ds(1 + 2 * p, 2)], as_sem.at[u], ar_sem.at[j], {"sp": mate})

    def a_outer(u):
        k, j = unit_home(u)
        return remote(asend.at[u, p], abuf.at[j, 5 * (1 - p)], os_sem.at[u], hr_sem.at[1 - p, j],
                      {"sp": 2 * near_q + lax.rem(k + near_q, 2)})

    def a_halo(i, t):
        j = SOLO // 4 + t
        return remote(abuf.at[j, 1 + 3 * i], abuf.at[j, 5 * (1 - i)], hs_sem.at[i, t], hr_sem.at[1 - i, j],
                      {"sp": s - 2 * p - 1 + 4 * i})

    def halo_arrived(i, j):
        return remote(abuf.at[0, 0], abuf.at[j, 5 * i], hs_sem.at[0, 0], hr_sem.at[i, j], {"sp": mate})

    def mate_sum(m):
        return remote(msend.at[m], mrecv.at[m], ms_sem.at[m], mr_sem.at[m], {"sp": mate})

    for g in range(SLOTS):
        fetch(jnp.int32(g))
    x_copies = [pltpu.make_async_copy(x_ref.at[pl.ds(h * ROW, ROW)], xbuf.at[1 + 2 * p + h], xsem.at[h]) for h in range(2)]
    for x_copy in x_copies:
        x_copy.start()
    b_copy = pltpu.make_async_copy(bias_ref, bias_v, bsem)
    b_copy.start()

    has_far = ((p == 0) & has_bot) | ((p == 1) & has_top)
    barrier = pltpu.get_barrier_semaphore()

    def greet(device_id):
        pl.semaphore_signal(barrier, inc=1, device_id=device_id, device_id_type=MESH)

    greet({"cp": other})
    greet({"sp": mate})

    @pl.when(has_near)
    def _():
        for k in range(2):
            greet({"sp": 2 * near_q + k})

    @pl.when(has_far)
    def _():
        for k in range(2):
            greet({"sp": s + (2 + k) * (1 - 2 * p)})

    pl.semaphore_wait(barrier, 2 + 2 * has_near.astype(jnp.int32) + 2 * has_far.astype(jnp.int32))

    x_mate(0).start()

    @pl.when(has_near)
    def _():
        x_outer().start()

    x_mate(1).start()

    zero = jnp.zeros((ROW, CHUNK), jnp.bfloat16)

    def clear_row(r):
        for k in range(half_o // CHUNK):
            xbuf[r, :, pl.ds(k * CHUNK, CHUNK)] = zero
        for j in range(4):
            abuf[j, r] = zero

    @pl.when(jnp.logical_not(has_top))
    def _():
        clear_row(0)

    @pl.when(jnp.logical_not(has_bot))
    def _():
        clear_row(5)

    b_copy.wait()
    for x_copy in x_copies:
        x_copy.wait()

    def group(slot, lhs, r0, nh, dst, d0, add, waiting=None):
        def wait():
            for kx, _, _, _ in TAPS:
                w_copy(w1_ref, kx, 0, 0, slot).wait()

        if waiting is None:
            wait()
        else:
            pl.when(waiting)(wait)
        for kx, src_col, dst_col, width in TAPS:
            total = None
            for ky in range(3):
                part = jnp.dot(lhs(r0 + ky, nh, src_col, width), wbuf[slot, kx, ky], preferred_element_type=jnp.float32)
                total = part if total is None else total + part
            total = total.reshape(nh, width, CHUNK)
            where = (pl.ds(d0, nh), pl.ds(dst_col, width), slice(None))
            if add or kx != 1:
                dst[where] = dst[where] + total
            else:
                dst[where] = total

    def x_lhs(r, nh, col, width):
        return xbuf[pl.ds(r, nh), pl.ds(col, width), :].reshape(nh * width, half_o)

    def bias_row(unit, n):
        return bias_v[pl.ds(c * (half_h // 128) + unit * (CHUNK // 128) + n, 1), :]

    def solo_step(g, carry):
        side = lax.rem(g, 2)
        u = g // 2
        dst = side * 2 + (1 - side) * u

        @pl.when(g == 0)
        def _():
            x_arrived(0).wait_recv()

            @pl.when(has_near)
            def _():
                x_arrived(2 + p).wait_recv()
                x_forward().start()

        group(lax.rem(g, SLOTS), x_lhs, 2 * p, 2, stage.at[dst], 0, False)
        fetch(g + SLOTS)

        @pl.when(side == 0)
        def _():
            solo_part(u).start()

        @pl.when(side == 1)
        def _():
            solo_part(u).wait_recv()
            k, j = unit_home(u)
            for h in range(2):
                for n in range(CHUNK // 128):
                    cols = pl.ds(n * 128, 128)
                    val = stage[2, h, :, cols] + recv1[u, h, :, cols] + bias_row(UNITS * k + j, n)
                    asend[u, h, :, cols] = jnp.maximum(val, 0.0).astype(jnp.bfloat16)

            @pl.when(k == share)
            def _():
                abuf[j, pl.ds(1 + 2 * p, 2)] = asend[u]

            @pl.when(k != share)
            def _():
                a_mate(u).start()

            @pl.when(has_near)
            def _():
                a_outer(u).start()
        return carry

    lax.fori_loop(0, SOLO, solo_step, 0)

    x_arrived(1).wait_recv()

    @pl.when(has_far)
    def _():
        x_arrived(3 - p).wait_recv()

    def shared_step(i, carry):
        side = lax.rem(i, 2)
        t = i // 2
        dst = side * 2 + (1 - side) * lax.rem(t, 2)

        @pl.when((side == 0) & (t < 2))
        def _():
            solo_part(t).wait_send()

        @pl.when((side == 0) & (t >= 2))
        def _():
            shared_part(t).wait_send()

        group(lax.rem(SOLO + i, SLOTS), x_lhs, 0, 4, stage.at[dst], 0, False)
        fetch(SOLO + i + SLOTS)

        @pl.when(side == 0)
        def _():
            shared_part(t).start()

        @pl.when(side == 1)
        def _():
            shared_part(t).wait_recv()
            for r in range(4):
                for n in range(CHUNK // 128):
                    cols = pl.ds(n * 128, 128)
                    val = stage[2, r, :, cols] + recv1[SOLO // 2 + 2 * t + r // 2, r % 2, :, cols] + bias_row(UNITS * share + SOLO // 4 + t, n)
                    abuf[SOLO // 4 + t, 1 + r, :, cols] = jnp.maximum(val, 0.0).astype(jnp.bfloat16)

            @pl.when(has_top)
            def _():
                a_halo(0, t).start()

            @pl.when(has_bot)
            def _():
                a_halo(1, t).start()
        return carry

    lax.fori_loop(0, SHARED, shared_step, 0)

    def a_lhs(kb):
        def lhs(r, nh, col, width):
            return jnp.concatenate([abuf[2 * kb + d, pl.ds(r, nh), pl.ds(col, width), :].reshape(nh * width, CHUNK)
                                    for d in range(2)], axis=1)
        return lhs

    def wait_a(kb):
        for d in range(2):
            j = 2 * kb + d
            if j < SOLO // 4:
                remote(asend.at[0], abuf.at[j, pl.ds(1, 2)], as_sem.at[0], ar_sem.at[j], {"sp": mate}).wait_recv()

            @pl.when(has_top)
            def _():
                halo_arrived(0, j).wait_recv()

            @pl.when(has_bot)
            def _():
                halo_arrived(1, j).wait_recv()

    for t in range(SHARED // 2 - 2, SHARED // 2):
        shared_part(jnp.int32(t)).wait_send()
    stage[...] = jnp.zeros((4, 4, ROW, CHUNK), jnp.float32)

    def second_step(i, carry):
        turn = i // 8
        t = lax.rem(i, 4)
        last = lax.rem(i // 4, 2)
        kb = lax.rem(turn + last, 2)
        m = t // 2
        side = lax.rem(t, 2)
        r0 = 2 * lax.rem(p + 1 + turn, 2)
        g = SECOND + i - 4 * turn

        for k in range(2):
            @pl.when(i == 4 * k)
            def _():
                wait_a(k)

        group(lax.rem(g, SLOTS), a_lhs(kb), r0, 2, stage.at[2 * side + m], 2 * turn, True, i // 4 != 2)

        @pl.when(i // 4 != 1)
        def _():
            fetch(g + SLOTS)

        @pl.when((last == 1) & (side == 0))
        def _():
            out_part(turn, m, r0).start()

        @pl.when((last == 1) & (side == 1))
        def _():
            out_part(turn, m, r0).wait_recv()

            @pl.when(turn == 0)
            def _():
                msend[m] = stage[2 + m, pl.ds(0, 2)] + recv2[m, pl.ds(r0, 2)]
                mate_sum(m).start()

            @pl.when(turn == 1)
            def _():
                mate_sum(m).wait_recv()
                cols = pl.ds(pl.multiple_of(m * CHUNK, CHUNK), CHUNK)
                for h in range(2):
                    total = stage[2 + m, 2 + h] + recv2[m, r0 + h] + mrecv[m, h]
                    out_ref[pl.ds(h * ROW, ROW), cols] = (xbuf[1 + 2 * p + h, :, cols].astype(jnp.float32) + total).astype(jnp.bfloat16)
        return carry

    lax.fori_loop(0, 16, second_step, 0)

    for m in range(2):
        for turn in range(2):
            out_part(turn, m, 0).wait_send()
        mate_sum(m).wait_send()
        x_mate(m).wait_send()

    def drain_solo(u, carry):
        k, _ = unit_home(u)

        @pl.when(k != share)
        def _():
            a_mate(u).wait_send()

        @pl.when(has_near)
        def _():
            a_outer(u).wait_send()
        return carry

    lax.fori_loop(0, SOLO // 2, drain_solo, 0)

    @pl.when(has_near)
    def _():
        x_outer().wait_send()
        x_forward().wait_send()

    for i, exists in enumerate((has_top, has_bot)):
        @pl.when(exists)
        def _():
            for t in range(SHARED // 2):
                a_halo(i, t).wait_send()


def solution(mesh):
    sp_size = mesh.shape["sp"]
    act_spec = P("dp", "sp", None, "cp")
    kernel_spec = P(None, None, "cp", None)

    def local_block(x_tile, w_one, w_two, bias):
        half_o, half_h = x_tile.shape[3], w_two.shape[2]
        x_rows = x_tile.transpose(1, 2, 0, 3).reshape(OWN, half_o)
        any_spec = pl.BlockSpec(memory_space=pl.ANY)
        dma = pltpu.SemaphoreType.DMA
        f32, bf16 = jnp.float32, jnp.bfloat16
        out = pl.pallas_call(
            functools.partial(resblock_kernel, sp_size, half_o, half_h),
            out_shape=jax.ShapeDtypeStruct((OWN, half_o), bf16),
            in_specs=[any_spec] * 4,
            out_specs=pl.BlockSpec(memory_space=pltpu.VMEM),
            scratch_shapes=[
                pltpu.VMEM((6, ROW, half_o), bf16),
                pltpu.VMEM((4, 6, ROW, CHUNK), bf16),
                pltpu.VMEM((SOLO // 2, 2, ROW, CHUNK), bf16),
                pltpu.VMEM((SLOTS, 3, 3, KBLOCK, CHUNK), bf16),
                pltpu.VMEM((4, 4, ROW, CHUNK), f32),
                pltpu.VMEM((8, 2, ROW, CHUNK), f32),
                pltpu.VMEM((2, 4, ROW, CHUNK), f32),
                pltpu.VMEM((2, 2, ROW, CHUNK), f32),
                pltpu.VMEM((2, 2, ROW, CHUNK), f32),
                pltpu.VMEM((2 * half_h // 128, 128), f32),
                dma((SLOTS, 3)), dma((2,)), dma, dma((4,)), dma((4,)), dma((2,)), dma(((SOLO + SHARED) // 2,)), dma((2, 2)), dma((2, 2)),
                dma((SOLO // 2,)), dma((SOLO // 4,)), dma((SOLO // 2,)), dma((2, SHARED // 2)), dma((2, 4)), dma((2,)), dma((2,)),
            ],
            compiler_params=pltpu.CompilerParams(
                collective_id=0, has_side_effects=True, vmem_limit_bytes=53 * 1024 * 1024),
        )(x_rows, w_one, w_two, bias.reshape(2 * half_h // 128, 128))
        return out.reshape(2, COLS, IMAGES, half_o).transpose(2, 0, 1, 3)

    return jax.shard_map(local_block, mesh=mesh, in_specs=(act_spec, kernel_spec, kernel_spec, P(None)), out_specs=act_spec, check_vma=False)
```

```python
import functools

import jax
import jax.numpy as jnp
from jax import lax
from jax.experimental import pallas as pl
from jax.experimental.pallas import tpu as pltpu
from jax.sharding import PartitionSpec as P

IMAGES = 16
COLS = 7
ROW = COLS * IMAGES
SIDE = ROW - IMAGES
OWN = 2 * ROW
CHUNK = 512
KBLOCK = 1024
SLOTS = 4
SOLO = 4
SHARED = 6
UNITS = 4
SECOND = SOLO + SHARED
GROUPS = SECOND + 12
MESH = pl.DeviceIdType.MESH
TAPS = ((1, 0, 0, ROW), (0, 0, IMAGES, SIDE), (2, IMAGES, 0, SIDE))


def resblock_kernel(sp_size, half_o, half_h, x_ref, w1_ref, w2_ref, bias_ref, out_ref,
                    xbuf, abuf, asend, wbuf, stage, recv1, recv2, msend, mrecv, bias_v,
                    wsem, xsem, bsem, xs_sem, xr_sem, ps_sem, pr1_sem, po_sem, pr2_sem,
                    as_sem, ar_sem, os_sem, hs_sem, hr_sem, ms_sem, mr_sem):
    c = lax.axis_index("cp")
    s = lax.axis_index("sp")
    other = 1 - c
    p = lax.rem(s, 2)
    q = s // 2
    mate = s + 1 - 2 * p
    has_top = q > 0
    has_bot = q < sp_size // 2 - 1
    has_near = (s > 0) & (s < sp_size - 1)
    near_q = q + 2 * p - 1
    share = lax.rem(p + q, 2)

    def w_copy(ref, kx, rows, cols, slot):
        return pltpu.make_async_copy(
            ref.at[:, kx, pl.ds(rows, KBLOCK), pl.ds(cols, CHUNK)], wbuf.at[slot, kx], wsem.at[slot, kx])

    def fetch(g):
        slot = lax.rem(g, SLOTS)

        @pl.when(g < SECOND)
        def _():
            side = lax.rem(g, 2)
            u = g // 2
            shared = (g + SECOND - SOLO) // SECOND
            unit = (1 - shared) * (UNITS * lax.rem(u, 2) + u // 2) + shared * (UNITS * share + u - SOLO // 4)
            cols = (side * c + (1 - side) * other) * half_h + unit * CHUNK
            for kx, _, _, _ in TAPS:
                w_copy(w1_ref, kx, 0, pl.multiple_of(cols, CHUNK), slot).start(priority=1)

        @pl.when((g >= SECOND) & (g < GROUPS))
        def _():
            t = g - SECOND
            kb = lax.rem(t // 4, 2)
            m = lax.rem(t, 4) // 2
            side = lax.rem(t, 2)
            cols = (side * c + (1 - side) * other) * half_o + m * CHUNK
            rows = share * 2 * KBLOCK + kb * KBLOCK
            for kx, _, _, _ in TAPS:
                w_copy(w2_ref, kx, pl.multiple_of(rows, KBLOCK), pl.multiple_of(cols, CHUNK), slot).start(priority=1)

    def remote(src, dst, send_sem, recv_sem, device_id):
        return pltpu.make_async_remote_copy(src, dst, send_sem, recv_sem, device_id=device_id, device_id_type=MESH)

    def x_mate(i):
        row = 1 - p if i == 0 else p
        return remote(x_ref.at[pl.ds(row * ROW, ROW)], xbuf.at[1 + 2 * p + row], xs_sem.at[i], xr_sem.at[i], {"sp": mate})

    def x_outer():
        return remote(x_ref.at[pl.ds(p * ROW, ROW)], xbuf.at[5 * (1 - p)], xs_sem.at[2], xr_sem.at[3 - p],
                      {"sp": 2 * near_q + 1 - p})

    def x_forward():
        return remote(xbuf.at[5 * p], xbuf.at[5 * p], xs_sem.at[3], xr_sem.at[2 + p], {"sp": mate})

    def x_arrived(i):
        return remote(x_ref.at[pl.ds(0, ROW)], xbuf.at[0], xs_sem.at[0], xr_sem.at[i], {"sp": mate})

    def part_send(src, dst, ssem, rsem):
        return remote(src, dst, ssem, rsem, {"cp": other})

    def solo_part(u):
        return part_send(stage.at[lax.rem(u, 2), pl.ds(0, 2)], recv1.at[u], ps_sem.at[lax.rem(u, 2)], pr1_sem.at[u])

    def shared_part(t):
        slot = lax.rem(t, 2)
        return part_send(stage.at[slot].reshape(2, 2, ROW, CHUNK), recv1.at[pl.ds(SOLO // 2 + 2 * t, 2)],
                         ps_sem.at[slot], pr1_sem.at[SOLO // 2 + t])

    def out_part(turn, m, r0):
        return part_send(stage.at[m, pl.ds(2 * turn, 2)], recv2.at[m, pl.ds(r0, 2)], po_sem.at[turn, m], pr2_sem.at[turn, m])

    def unit_home(u):
        return lax.rem(u, 2), u // 2

    def a_mate(u):
        _, j = unit_home(u)
        return remote(asend.at[u], abuf.at[j, pl.ds(1 + 2 * p, 2)], as_sem.at[u], ar_sem.at[j], {"sp": mate})

    def a_outer(u):
        k, j = unit_home(u)
        return remote(asend.at[u, p], abuf.at[j, 5 * (1 - p)], os_sem.at[u], hr_sem.at[1 - p, j],
                      {"sp": 2 * near_q + lax.rem(k + near_q, 2)})

    def a_halo(i, t):
        j = SOLO // 4 + t
        return remote(abuf.at[j, 1 + 3 * i], abuf.at[j, 5 * (1 - i)], hs_sem.at[i, t], hr_sem.at[1 - i, j],
                      {"sp": s - 2 * p - 1 + 4 * i})

    def halo_arrived(i, j):
        return remote(abuf.at[0, 0], abuf.at[j, 5 * i], hs_sem.at[0, 0], hr_sem.at[i, j], {"sp": mate})

    def mate_sum(m):
        return remote(msend.at[m], mrecv.at[m], ms_sem.at[m], mr_sem.at[m], {"sp": mate})

    x_copies = [pltpu.make_async_copy(x_ref.at[pl.ds(h * ROW, ROW)], xbuf.at[1 + 2 * p + h], xsem.at[h]) for h in range(2)]
    for x_copy in x_copies:
        x_copy.start()
    b_copy = pltpu.make_async_copy(bias_ref, bias_v, bsem)
    b_copy.start()
    for g in range(SLOTS):
        fetch(jnp.int32(g))

    has_far = ((p == 0) & has_bot) | ((p == 1) & has_top)
    barrier = pltpu.get_barrier_semaphore()

    def greet(device_id):
        pl.semaphore_signal(barrier, inc=1, device_id=device_id, device_id_type=MESH)

    greet({"cp": other})
    greet({"sp": mate})

    @pl.when(has_near)
    def _():
        for k in range(2):
            greet({"sp": 2 * near_q + k})

    @pl.when(has_far)
    def _():
        for k in range(2):
            greet({"sp": s + (2 + k) * (1 - 2 * p)})

    pl.semaphore_wait(barrier, 2 + 2 * has_near.astype(jnp.int32) + 2 * has_far.astype(jnp.int32))

    x_mate(0).start()

    @pl.when(has_near)
    def _():
        x_outer().start()

    x_mate(1).start()

    zero = jnp.zeros((ROW, CHUNK), jnp.bfloat16)

    def clear_row(r):
        for k in range(half_o // CHUNK):
            xbuf[r, :, pl.ds(k * CHUNK, CHUNK)] = zero
        for j in range(4):
            abuf[j, r] = zero

    @pl.when(jnp.logical_not(has_top))
    def _():
        clear_row(0)

    @pl.when(jnp.logical_not(has_bot))
    def _():
        clear_row(5)

    b_copy.wait()
    for x_copy in x_copies:
        x_copy.wait()

    def group(slot, lhs, r0, nh, dst, d0, add, waiting=None):
        def wait():
            for kx, _, _, _ in TAPS:
                w_copy(w1_ref, kx, 0, 0, slot).wait()

        if waiting is None:
            wait()
        else:
            pl.when(waiting)(wait)
        for kx, src_col, dst_col, width in TAPS:
            total = None
            for ky in range(3):
                part = jnp.dot(lhs(r0 + ky, nh, src_col, width), wbuf[slot, kx, ky], preferred_element_type=jnp.float32)
                total = part if total is None else total + part
            total = total.reshape(nh, width, CHUNK)
            where = (pl.ds(d0, nh), pl.ds(dst_col, width), slice(None))
            if add or kx != 1:
                dst[where] = dst[where] + total
            else:
                dst[where] = total

    def x_lhs(r, nh, col, width):
        return xbuf[pl.ds(r, nh), pl.ds(col, width), :].reshape(nh * width, half_o)

    def bias_row(unit, n):
        return bias_v[pl.ds(c * (half_h // 128) + unit * (CHUNK // 128) + n, 1), :]

    def solo_step(g, carry):
        side = lax.rem(g, 2)
        u = g // 2
        dst = side * 2 + (1 - side) * u

        @pl.when(g == 0)
        def _():
            x_arrived(0).wait_recv()

            @pl.when(has_near)
            def _():
                x_arrived(2 + p).wait_recv()
                x_forward().start()

        group(lax.rem(g, SLOTS), x_lhs, 2 * p, 2, stage.at[dst], 0, False)
        fetch(g + SLOTS)

        @pl.when(side == 0)
        def _():
            solo_part(u).start()

        @pl.when(side == 1)
        def _():
            solo_part(u).wait_recv()
            k, j = unit_home(u)
            for h in range(2):
                for n in range(CHUNK // 128):
                    cols = pl.ds(n * 128, 128)
                    val = stage[2, h, :, cols] + recv1[u, h, :, cols] + bias_row(UNITS * k + j, n)
                    asend[u, h, :, cols] = jnp.maximum(val, 0.0).astype(jnp.bfloat16)

            @pl.when(k == share)
            def _():
                abuf[j, pl.ds(1 + 2 * p, 2)] = asend[u]

            @pl.when(k != share)
            def _():
                a_mate(u).start()

            @pl.when(has_near)
            def _():
                a_outer(u).start()
        return carry

    lax.fori_loop(0, SOLO, solo_step, 0)

    x_arrived(1).wait_recv()

    @pl.when(has_far)
    def _():
        x_arrived(3 - p).wait_recv()

    def shared_step(i, carry):
        side = lax.rem(i, 2)
        t = i // 2
        dst = side * 2 + (1 - side) * lax.rem(t, 2)

        @pl.when((side == 0) & (t < 2))
        def _():
            solo_part(t).wait_send()

        @pl.when((side == 0) & (t >= 2))
        def _():
            shared_part(t).wait_send()

        group(lax.rem(SOLO + i, SLOTS), x_lhs, 0, 4, stage.at[dst], 0, False)
        fetch(SOLO + i + SLOTS)

        @pl.when(side == 0)
        def _():
            shared_part(t).start()

        @pl.when(side == 1)
        def _():
            shared_part(t).wait_recv()
            for r in range(4):
                for n in range(CHUNK // 128):
                    cols = pl.ds(n * 128, 128)
                    val = stage[2, r, :, cols] + recv1[SOLO // 2 + 2 * t + r // 2, r % 2, :, cols] + bias_row(UNITS * share + SOLO // 4 + t, n)
                    abuf[SOLO // 4 + t, 1 + r, :, cols] = jnp.maximum(val, 0.0).astype(jnp.bfloat16)

            @pl.when(has_top)
            def _():
                a_halo(0, t).start()

            @pl.when(has_bot)
            def _():
                a_halo(1, t).start()
        return carry

    lax.fori_loop(0, SHARED, shared_step, 0)

    def a_lhs(kb):
        def lhs(r, nh, col, width):
            return jnp.concatenate([abuf[2 * kb + d, pl.ds(r, nh), pl.ds(col, width), :].reshape(nh * width, CHUNK)
                                    for d in range(2)], axis=1)
        return lhs

    def wait_a(kb):
        for d in range(2):
            j = 2 * kb + d
            if j < SOLO // 4:
                remote(asend.at[0], abuf.at[j, pl.ds(1, 2)], as_sem.at[0], ar_sem.at[j], {"sp": mate}).wait_recv()

            @pl.when(has_top)
            def _():
                halo_arrived(0, j).wait_recv()

            @pl.when(has_bot)
            def _():
                halo_arrived(1, j).wait_recv()

    for t in range(SHARED // 2 - 2, SHARED // 2):
        shared_part(jnp.int32(t)).wait_send()
    stage[...] = jnp.zeros((4, 4, ROW, CHUNK), jnp.float32)

    def second_step(i, carry):
        turn = i // 8
        t = lax.rem(i, 4)
        last = lax.rem(i // 4, 2)
        kb = lax.rem(turn + last, 2)
        m = t // 2
        side = lax.rem(t, 2)
        r0 = 2 * lax.rem(p + 1 + turn, 2)
        g = SECOND + i - 4 * turn

        for k in range(2):
            @pl.when(i == 4 * k)
            def _():
                wait_a(k)

        group(lax.rem(g, SLOTS), a_lhs(kb), r0, 2, stage.at[2 * side + m], 2 * turn, True, i // 4 != 2)

        @pl.when(i // 4 != 1)
        def _():
            fetch(g + SLOTS)

        @pl.when((last == 1) & (side == 0))
        def _():
            out_part(turn, m, r0).start()

        @pl.when((last == 1) & (side == 1))
        def _():
            out_part(turn, m, r0).wait_recv()

            @pl.when(turn == 0)
            def _():
                msend[m] = stage[2 + m, pl.ds(0, 2)] + recv2[m, pl.ds(r0, 2)]
                mate_sum(m).start()

            @pl.when(turn == 1)
            def _():
                mate_sum(m).wait_recv()
                cols = pl.ds(pl.multiple_of(m * CHUNK, CHUNK), CHUNK)
                for h in range(2):
                    total = stage[2 + m, 2 + h] + recv2[m, r0 + h] + mrecv[m, h]
                    out_ref[pl.ds(h * ROW, ROW), cols] = (xbuf[1 + 2 * p + h, :, cols].astype(jnp.float32) + total).astype(jnp.bfloat16)
        return carry

    lax.fori_loop(0, 16, second_step, 0)

    for m in range(2):
        for turn in range(2):
            out_part(turn, m, 0).wait_send()
        mate_sum(m).wait_send()
        x_mate(m).wait_send()

    def drain_solo(u, carry):
        k, _ = unit_home(u)

        @pl.when(k != share)
        def _():
            a_mate(u).wait_send()

        @pl.when(has_near)
        def _():
            a_outer(u).wait_send()
        return carry

    lax.fori_loop(0, SOLO // 2, drain_solo, 0)

    @pl.when(has_near)
    def _():
        x_outer().wait_send()
        x_forward().wait_send()

    for i, exists in enumerate((has_top, has_bot)):
        @pl.when(exists)
        def _():
            for t in range(SHARED // 2):
                a_halo(i, t).wait_send()


def solution(mesh):
    sp_size = mesh.shape["sp"]
    act_spec = P("dp", "sp", None, "cp")
    kernel_spec = P(None, None, "cp", None)

    def local_block(x_tile, w_one, w_two, bias):
        half_o, half_h = x_tile.shape[3], w_two.shape[2]
        x_rows = x_tile.transpose(1, 2, 0, 3).reshape(OWN, half_o)
        any_spec = pl.BlockSpec(memory_space=pl.ANY)
        dma = pltpu.SemaphoreType.DMA
        f32, bf16 = jnp.float32, jnp.bfloat16
        out = pl.pallas_call(
            functools.partial(resblock_kernel, sp_size, half_o, half_h),
            out_shape=jax.ShapeDtypeStruct((OWN, half_o), bf16),
            in_specs=[any_spec] * 4,
            out_specs=pl.BlockSpec(memory_space=pltpu.VMEM),
            scratch_shapes=[
                pltpu.VMEM((6, ROW, half_o), bf16),
                pltpu.VMEM((4, 6, ROW, CHUNK), bf16),
                pltpu.VMEM((SOLO // 2, 2, ROW, CHUNK), bf16),
                pltpu.VMEM((SLOTS, 3, 3, KBLOCK, CHUNK), bf16),
                pltpu.VMEM((4, 4, ROW, CHUNK), f32),
                pltpu.VMEM((8, 2, ROW, CHUNK), f32),
                pltpu.VMEM((2, 4, ROW, CHUNK), f32),
                pltpu.VMEM((2, 2, ROW, CHUNK), f32),
                pltpu.VMEM((2, 2, ROW, CHUNK), f32),
                pltpu.VMEM((2 * half_h // 128, 128), f32),
                dma((SLOTS, 3)), dma((2,)), dma, dma((4,)), dma((4,)), dma((2,)), dma(((SOLO + SHARED) // 2,)), dma((2, 2)), dma((2, 2)),
                dma((SOLO // 2,)), dma((SOLO // 4,)), dma((SOLO // 2,)), dma((2, SHARED // 2)), dma((2, 4)), dma((2,)), dma((2,)),
            ],
            compiler_params=pltpu.CompilerParams(
                collective_id=0, has_side_effects=True, vmem_limit_bytes=53 * 1024 * 1024),
        )(x_rows, w_one, w_two, bias.reshape(2 * half_h // 128, 128))
        return out.reshape(2, COLS, IMAGES, half_o).transpose(2, 0, 1, 3)

    return jax.shard_map(local_block, mesh=mesh, in_specs=(act_spec, kernel_spec, kernel_spec, P(None)), out_specs=act_spec, check_vma=False)
```
